32 devices in a mesh: row: 2 (over core), col: 4 (over y, x), exp: 4 (over z).
Axes of the slice: x: 2, y: 2, z: 4, core: 2. Of those that a mesh axis runs over, the one named last changes fastest.
Arguments:
- tokens: bfloat16 [4, 2048, 1024], P('exp', ('row', 'col')), may hold values from -6 to 6
- seg_ids: int32 [4, 2048], P('exp'), may hold values from 0 to 7, never falling along the last dimension, each value on 1 to 1536 neighbouring positions
- routes: int32 [4, 2048, 8], P('exp', ('row', 'col')), may hold values from 0 to 31, all different within a row
- priority: int32 [4, 2048], P('exp', ('row', 'col')), may hold values from 0 to 255, as said below
- cotangent: bfloat16 [4, 2048, 1024], P('exp', ('row', 'col')), may hold values from -6 to 6
- norm1_gain: bfloat16 [1024], replicated, may hold values from 0.5 to 1.5
- w_query: bfloat16 [1024, 1024], P(None, 'col'), may hold values from -0.1875 to 0.1875
- key_projection: bfloat16 [1024, 512], P(None, 'col'), may hold values from -0.1875 to 0.1875
- value_projection: bfloat16 [1024, 512], P(None, 'col'), may hold values from -0.1875 to 0.1875
- w_out: bfloat16 [1024, 1024], P('col'), may hold values from -0.75 to 0.75
- norm2_gain: bfloat16 [1024], replicated, may hold values from 0.5 to 1.5
- w_router: bfloat16 [1024, 32], replicated, may hold values from -0.375 to 0.375
- w_gate: bfloat16 [32, 1024, 512], P('exp'), may hold values from -0.1875 to 0.1875
- w_up: bfloat16 [32, 1024, 512], P('exp'), may hold values from -0.1875 to 0.1875
- w_down: bfloat16 [32, 512, 1024], P('exp'), may hold values from -0.5 to 0.5
Outputs:
- output: bfloat16 [4, 2048, 1024], P('exp', ('row', 'col'))
- input_gradient: float32 [4, 2048, 1024], P('exp', ('row', 'col'))
- norm1_gain_grad: float32 [1024], P('col')
- w_query_grad: float32 [1024, 1024], P(None, 'col')
- w_key_grad: float32 [1024, 512], P(None, 'col')
- w_value_grad: float32 [1024, 512], P(None, 'col')
- w_out_grad: float32 [1024, 1024], P('col')
- norm2_gain_grad: float32 [1024], P('col')
- w_router_grad: float32 [1024, 32], P('col')
- w_gate_grad: float32 [32, 1024, 512], P('exp', ('row', 'col'))
- w_up_grad: float32 [32, 1024, 512], P('exp', ('row', 'col'))
- w_down_grad: float32 [32, 512, 1024], P('exp', ('row', 'col'))
The draws below stay inside these ranges and needn't reach their ends.
Inputs may be any that keep to these rules, and one draw needn't show every extreme that they name: `seg_ids`: segment numbers never fall along a sequence; a document (a run of equal numbers) has at most 1536 positions. `routes`: each token names 8 different experts. `priority`: within every aligned block of 256 positions of a sequence the values are a permutation of 0 to 255.
All inputs are finite; a program needn't handle non-finite values.
Results may differ from the reference program's by a relative error of at most 0.024.
Values may be sent and summed in bfloat16 or wider, within the bound.
A program may use at most 192 MiB of HBM per device.

```python
import math
import jax
import jax.numpy as jnp
import numpy as np
from jax import lax

MODEL_DIM = 1024
QUERY_HEADS = 16
KEY_VALUE_HEADS = 8
HEAD_SIZE = 64
EXPERTS = 32
F = 512
TOP = 8
ROWS = 256
LENGTH = 2048
SEQS = 4
CAP = 72
DOCS = 8
LONGEST = 1536


def draw_priority(key, part):
    blocks = SEQS * LENGTH // ROWS
    sub_keys = jax.random.split(key, blocks)

    def permute(sub_key):
        return jax.random.permutation(sub_key, ROWS)
    orders = jax.vmap(permute)(sub_keys)
    return orders.reshape(SEQS, LENGTH).astype(jnp.int32)


def with_spikes(array, rng, source, target, parts, factor):
    owner, partner = [(jnp.arange(array.shape[axis_at]) // (array.shape[axis_at] // parts)).reshape([-1 if axis == axis_at else 1 for axis in range(array.ndim)]) for axis_at in (source, target)]
    chosen = jax.random.permutation(rng, parts)[partner]
    strong = (owner == chosen) | (owner == (partner + parts // 2) % parts)
    return jnp.where(strong, factor * array, array)


def block_levels(stream_key, extent, shards, low, top_value):
    factor_of = 1.0
    for axis_at, shards_of in shards:
        heights = jax.random.uniform(jax.random.fold_in(jax.random.fold_in(stream_key, 6), axis_at), (shards_of,), jnp.float32, low / len(shards), top_value / len(shards))
        factor_of = factor_of * jnp.repeat(jnp.exp(heights), extent[axis_at] // shards_of).reshape((-1,) + (1,) * (len(extent) - 1 - axis_at))
    return factor_of


def choose_distinct(rng, rows, number_of, top, lift):
    ranking = jax.random.permutation(jax.random.fold_in(rng, 1), number_of)
    pull = ranking
    for power in range(3):
        pull = pull * pull // number_of
    pull = pull * lift // number_of
    lots = jax.random.randint(jax.random.fold_in(rng, 2), (rows, number_of), 0, 4096) + pull
    fixed_rows = jax.random.permutation(jax.random.fold_in(rng, 3), rows)[jnp.arange(number_of) % rows]
    lots = jnp.where(jnp.arange(rows)[:, None] == fixed_rows[None, :], 1 << 14, lots)
    score = lots * number_of + jnp.arange(number_of)
    return lax.top_k(score.astype(jnp.int32), top)[1].astype(jnp.int32)


def split_up(number_of, total, reach, lean):
    portions = [(1 << 20) // math.isqrt(rank ** lean) + 1 for rank in range(2, number_of + 1)]
    spare, given = total - reach - (number_of - 1), [1] * (number_of - 1)
    while spare > 0:
        free = [i for i in range(number_of - 1) if given[i] < reach]
        whole, remaining = sum([portions[i] for i in free]), spare
        for i in free:
            more = min(reach - given[i], max(1, remaining * portions[i] // whole), spare)
            given[i] = given[i] + more
            spare = spare - more
    return np.array([reach] + given)


def ragged_sizes(own_key, number_of, total, most, lean):
    if number_of == 2:
        one = jax.random.randint(own_key, (), max(1, total - most), min(most, total - 1) + 1)
        return jnp.stack([one, total - one])
    lengths = jnp.asarray(split_up(number_of, total, most, lean), jnp.int32)
    pairs = (number_of - 1) // 2
    donor, sink = lengths[1:1 + 2 * pairs:2], lengths[2:2 + 2 * pairs:2]
    margin = jnp.minimum(donor - 1, most - sink)
    shifted = jax.random.randint(jax.random.fold_in(own_key, 1), (pairs,), 0, 1 << 20) % (margin + 1)
    lengths = lengths.at[1:1 + 2 * pairs:2].set(donor - shifted).at[2:2 + 2 * pairs:2].set(sink + shifted)
    return lengths[jax.random.permutation(jax.random.fold_in(own_key, 2), number_of)]


def centred(stream_key, shape, scale, limit, cuts=(), held_as=jnp.bfloat16):
    values = scale * jax.random.normal(stream_key, shape, jnp.float32)
    if cuts:
        values = values * block_levels(stream_key, shape, cuts, -0.22, 0.18)
    return jnp.clip(values, -limit, limit).astype(held_as)


def gaussian_with(stream_key, extent, width, limit, shards, heavy, held_as=jnp.bfloat16):
    values = width * jax.random.normal(stream_key, extent, jnp.float32)
    if shards:
        values = values * block_levels(stream_key, extent, shards, -0.22, 0.18)
    return jnp.clip(with_spikes(values, jax.random.fold_in(stream_key, 3), *heavy), -limit, limit).astype(held_as)


def setup_inputs(seed: int = 0) -> dict:
    arg_keys = jax.random.split(jax.random.key(seed), 16)
    tokens = gaussian_with(arg_keys[0], (SEQS, LENGTH, MODEL_DIM), 1.0, 6.0, ((0, 4), (1, 8)), (1, 2, 8, 2.0))
    seg_ids = jax.vmap(lambda own: jnp.searchsorted(jnp.cumsum(ragged_sizes(own, DOCS, LENGTH, LONGEST, 2)), jnp.arange(LENGTH), side="right"))(jax.random.split(arg_keys[1], SEQS)).reshape((SEQS, LENGTH)).astype(jnp.int32)
    routes = choose_distinct(arg_keys[2], SEQS * LENGTH, EXPERTS, TOP, 2048).reshape((SEQS, LENGTH, TOP))
    priority = draw_priority(jax.random.fold_in(arg_keys[15], 71), 0)
    cotangent = centred(arg_keys[4], (SEQS, LENGTH, MODEL_DIM), 1.0, 6.0, ((0, 4), (1, 8)))
    norm1_gain = jnp.clip(1.0 + 0.1 * jax.random.normal(arg_keys[5], (MODEL_DIM,), jnp.float32), 0.5, 1.5).astype(jnp.bfloat16)
    w_query = centred(arg_keys[6], (MODEL_DIM, QUERY_HEADS * HEAD_SIZE), MODEL_DIM ** -0.5, 0.1875, ((1, 4),))
    key_projection = centred(arg_keys[7], (MODEL_DIM, KEY_VALUE_HEADS * HEAD_SIZE), MODEL_DIM ** -0.5, 0.1875, ((1, 4),))
    value_projection = centred(arg_keys[8], (MODEL_DIM, KEY_VALUE_HEADS * HEAD_SIZE), MODEL_DIM ** -0.5, 0.1875, ((1, 4),))
    w_out = centred(arg_keys[9], (QUERY_HEADS * HEAD_SIZE, MODEL_DIM), (MODEL_DIM // 16) ** -0.5, 0.75, ((0, 4),))
    norm2_gain = jnp.clip(1.0 + 0.1 * jax.random.normal(arg_keys[10], (MODEL_DIM,), jnp.float32), 0.5, 1.5).astype(jnp.bfloat16)
    w_router = centred(arg_keys[11], (MODEL_DIM, EXPERTS), (MODEL_DIM // 4) ** -0.5, 0.375)
    w_gate = centred(arg_keys[12], (EXPERTS, MODEL_DIM, F), MODEL_DIM ** -0.5, 0.1875, ((0, 4),))
    w_up = centred(arg_keys[13], (EXPERTS, MODEL_DIM, F), MODEL_DIM ** -0.5, 0.1875, ((0, 4),))
    w_down = centred(arg_keys[14], (EXPERTS, F, MODEL_DIM), (F // 4) ** -0.5, 0.5, ((0, 4),))
    return dict(tokens=tokens, seg_ids=seg_ids, routes=routes, priority=priority, cotangent=cotangent, norm1_gain=norm1_gain, w_query=w_query, key_projection=key_projection, value_projection=value_projection, w_out=w_out, norm2_gain=norm2_gain, w_router=w_router, w_gate=w_gate, w_up=w_up, w_down=w_down)


EPS = 1e-06
THETA = 10000.0
HIGH = lax.Precision.HIGHEST
NEG = -1e+30

@jax.custom_vjp
def lower_precision(v):
    return lax.optimization_barrier(v.astype(jnp.bfloat16)).astype(jnp.float32)

@jax.custom_vjp
def low_back(v):
    return v

def low_keep(v):
    return (lower_precision(v), None)

def low_pass(kept, grad):
    return (grad,)

def back_keep(v):
    return (v, None)

def back_low(kept, grad):
    return (lower_precision(grad),)
lower_precision.defvjp(low_keep, low_pass)
low_back.defvjp(back_keep, back_low)

def matmul(left, right):
    return jnp.dot(left, right, precision=HIGH)

def angle_tables(count_rows):
    places = jnp.arange(count_rows).astype(jnp.float32)
    half_dim = HEAD_SIZE // 2
    frequency = THETA ** (-(jnp.arange(half_dim).astype(jnp.float32) * 2.0 / HEAD_SIZE))
    angles = places[:, None] * frequency[None, :]
    return (jnp.cos(angles), jnp.sin(angles))

def apply_rotation(values, cosine_table, sine_table):
    half_dim = values.shape[-1] // 2
    front_half = values[..., :half_dim]
    back_half = values[..., half_dim:]
    cos_b = cosine_table[:, None, :]
    sin_b = sine_table[:, None, :]
    return jnp.concatenate([front_half * cos_b - back_half * sin_b, back_half * cos_b + front_half * sin_b], axis=-1)

def rms_normed(values, gain_vector):
    inverse_norm = lax.rsqrt(lax.optimization_barrier(jnp.mean(values * values, axis=-1, keepdims=True)) + EPS)
    return values * inverse_norm * gain_vector

def swiglu(gate_val, up_val):
    return jax.nn.silu(gate_val) * up_val

def attend(rotated_query, rotated_key, reshaped_value, segment):
    sequence_length = rotated_query.shape[0]
    rows_per_tile = min(512, sequence_length)
    tile_number = sequence_length // rows_per_tile
    shared_token_count = QUERY_HEADS // KEY_VALUE_HEADS
    positions = jnp.arange(sequence_length, dtype=jnp.int32)

    def one_tile(pieces):
        q_tile, seg_tile, place_tile = pieces
        scores = jnp.einsum('qgrd,kgd->grqk', q_tile, rotated_key, precision=HIGH) * HEAD_SIZE ** (-0.5)
        scores = low_back(scores)
        allowed = (seg_tile[:, None] == segment[None, :]) & (positions[None, :] <= place_tile[:, None])
        scores = jnp.where(allowed, scores, NEG)
        top_score = lax.optimization_barrier(jnp.max(scores, axis=-1, keepdims=True))
        raised = jnp.where(allowed, jnp.exp(scores - top_score), 0.0)
        probabilities = lower_precision(raised / lax.optimization_barrier(jnp.sum(raised, axis=-1, keepdims=True)))
        return jnp.einsum('grqk,kgd->qgrd', probabilities, reshaped_value, precision=HIGH)
    query_tile_count = rotated_query.reshape(tile_number, rows_per_tile, KEY_VALUE_HEADS, shared_token_count, HEAD_SIZE)
    result = lax.map(jax.checkpoint(one_tile), (query_tile_count, segment.reshape(tile_number, rows_per_tile), positions.reshape(tile_number, rows_per_tile)))
    return result.reshape(sequence_length, QUERY_HEADS * HEAD_SIZE)

def expert_tile(tile_pieces, second_gain, router_w, gate_w, up_w, down_w):
    hidden_b, route_b, prio_b = tile_pieces
    normed = lower_precision(rms_normed(hidden_b, second_gain))
    logits = matmul(normed, router_w)
    picked = jnp.take_along_axis(logits, route_b, axis=1)
    gates = jax.nn.softmax(picked, axis=-1)
    expert_ids = jnp.arange(EXPERTS, dtype=jnp.int32)
    onehot = (route_b[:, :, None] == expert_ids[None, None, :]).astype(jnp.float32)
    counts = lax.optimization_barrier(jnp.sum(onehot, axis=1))
    earlier = (prio_b[None, :] < prio_b[:, None]).astype(jnp.float32)
    before = matmul(earlier, counts)
    slot_rank = lax.optimization_barrier(jnp.sum(onehot * before[:, None, :], axis=-1))
    is_kept = slot_rank < CAP
    slot_index = jnp.where(is_kept, route_b * CAP + slot_rank.astype(jnp.int32), EXPERTS * CAP)
    pair_count = ROWS * TOP
    slot_pair = jnp.full((EXPERTS * CAP,), pair_count, jnp.int32).at[slot_index.reshape(-1)].set(jnp.arange(pair_count, dtype=jnp.int32), mode='drop')
    slot_token = slot_pair // TOP
    padded = jnp.concatenate([normed, jnp.zeros((1, MODEL_DIM), jnp.float32)], axis=0)
    arrived = low_back(padded[slot_token]).reshape(EXPERTS, CAP, MODEL_DIM)
    gate_val = low_back(jnp.einsum('ecd,edf->ecf', arrived, gate_w, precision=HIGH))
    up_val = low_back(jnp.einsum('ecd,edf->ecf', arrived, up_w, precision=HIGH))
    activation = lower_precision(swiglu(gate_val, up_val))
    result = lower_precision(low_back(jnp.einsum('ecf,efd->ecd', activation, down_w, precision=HIGH)))
    padded_out = jnp.concatenate([result.reshape(EXPERTS * CAP, MODEL_DIM), jnp.zeros((1, MODEL_DIM), jnp.float32)], axis=0)
    picked_out = padded_out[slot_index]
    mixture = lax.optimization_barrier(jnp.sum(gates[:, :, None] * picked_out, axis=1))
    return hidden_b + mixture

def sequence_layer(pieces, params, cosine_table, sine_table):
    tokens_s, segment, route_s, prio_s = pieces
    first_gain, query_w, key_w, value_w, out_w, second_gain, router_w, gate_w, up_w, down_w = params
    sequence_length = tokens_s.shape[0]
    normed = lower_precision(rms_normed(tokens_s, first_gain))
    query = low_back(matmul(normed, query_w))
    unrotated_key = low_back(matmul(normed, key_w))
    unshaped_value = low_back(matmul(normed, value_w))
    rotated_query = lower_precision(apply_rotation(query.reshape(sequence_length, QUERY_HEADS, HEAD_SIZE), cosine_table, sine_table))
    rotated_key = lower_precision(apply_rotation(unrotated_key.reshape(sequence_length, KEY_VALUE_HEADS, HEAD_SIZE), cosine_table, sine_table))
    reshaped_value = lower_precision(unshaped_value.reshape(sequence_length, KEY_VALUE_HEADS, HEAD_SIZE))
    attended = lower_precision(low_back(attend(rotated_query, rotated_key, reshaped_value, segment)))
    branch = low_back(matmul(attended, out_w))
    hidden_state = tokens_s + branch
    blocks = sequence_length // ROWS

    def moe_tile(tile_pieces):
        return expert_tile(tile_pieces, second_gain, router_w, gate_w, up_w, down_w)
    mixed = lax.map(jax.checkpoint(moe_tile), (hidden_state.reshape(blocks, ROWS, MODEL_DIM), route_s.reshape(blocks, ROWS, TOP), prio_s.reshape(blocks, ROWS)))
    return mixed.reshape(sequence_length, MODEL_DIM)

def reference(tokens, seg_ids, routes, priority, cotangent, norm1_gain, w_query, key_projection, value_projection, w_out, norm2_gain, w_router, w_gate, w_up, w_down):
    cosine_table, sine_table = angle_tables(LENGTH)

    def forward(tokens_f, first_gain, query_w, key_w, value_w, out_w, second_gain, router_w, gate_w, up_w, down_w):
        params = (first_gain, query_w, key_w, value_w, out_w, second_gain, router_w, gate_w, up_w, down_w)

        def per_sequence(pieces):
            return sequence_layer(pieces, params, cosine_table, sine_table)
        return lax.map(per_sequence, (tokens_f, seg_ids, routes, priority))
    floats = (tokens.astype(jnp.float32), norm1_gain.astype(jnp.float32), w_query.astype(jnp.float32), key_projection.astype(jnp.float32), value_projection.astype(jnp.float32), w_out.astype(jnp.float32), norm2_gain.astype(jnp.float32), w_router.astype(jnp.float32), w_gate.astype(jnp.float32), w_up.astype(jnp.float32), w_down.astype(jnp.float32))
    result, pullback = jax.vjp(forward, *floats)
    grads = pullback(cotangent.astype(jnp.float32))
    return (result.astype(jnp.bfloat16), grads[0], grads[1], grads[2], grads[3], grads[4], grads[5], grads[6], grads[7], grads[8], grads[9], grads[10])
```

```python
import functools

import jax
import jax.numpy as jnp
from jax import lax
from jax.experimental import pallas as pl
from jax.experimental.pallas import tpu as pltpu
from jax.sharding import PartitionSpec as P

HEAD = 64
EPS = 1e-06
THETA = 10000.0
HIGH = lax.Precision.HIGHEST
NEG = -1e30
BK = 256
F32 = jnp.float32
BF16 = jnp.bfloat16
MESH = pl.DeviceIdType.MESH
VMEM_LIMIT = 66 * 1000 * 1000
VM = pl.BlockSpec(memory_space=pltpu.VMEM)
SM = pl.BlockSpec(memory_space=pltpu.SMEM)
ANY = pl.BlockSpec(memory_space=pl.ANY)


def dot(a, b, ca, cb):
    return lax.dot_general(a, b, (((ca,), (cb,)), ((), ())), preferred_element_type=F32)


def params(**kw):
    return pltpu.CompilerParams(vmem_limit_bytes=VMEM_LIMIT, **kw)


def cost(flops, nbytes, trans=0):
    return pl.CostEstimate(flops=int(flops), bytes_accessed=int(nbytes), transcendentals=int(trans))


def mate(c, j):
    y, x = c // 2, c % 2
    jy, jx = j // 2, j % 2
    return (y + jy - 2 * y * jy) * 2 + (x + jx - 2 * x * jx)


def col_swap(v, j):
    return lax.ppermute(v, "col", [(i, i ^ j) for i in range(4)])


def row_swap(v):
    return lax.ppermute(v, "row", [(0, 1), (1, 0)])


def cuts(rows, pieces):
    units = rows // 16
    if rows % 16 or units < pieces:
        return [(0, rows)]
    out, start = [], 0
    for i in range(pieces):
        size = (units // pieces + (1 if i < units % pieces else 0)) * 16
        out.append((start, size))
        start += size
    return out


def gather_kernel(nz, pieces, count, *refs):
    x_refs, out_refs = refs[:count], refs[count : 2 * count]
    send_r, recv_r, send_l, recv_l, send_c, recv_c, own_sem = refs[2 * count :]
    r, z = lax.axis_index("row"), lax.axis_index("exp")
    has_l, has_r = z > 0, z < nz - 1
    barrier = pltpu.get_barrier_semaphore()

    @pl.when(has_l)
    def _():
        pl.semaphore_signal(barrier, inc=1, device_id={"exp": z - 1}, device_id_type=MESH)

    @pl.when(has_r)
    def _():
        pl.semaphore_signal(barrier, inc=1, device_id={"exp": z + 1}, device_id_type=MESH)

    pl.semaphore_signal(barrier, inc=1, device_id={"row": 1 - r}, device_id_type=MESH)
    pl.semaphore_wait(barrier, 1 + has_l.astype(jnp.int32) + has_r.astype(jnp.int32))

    items = [(a, s, n) for a in range(count) for s, n in pieces[a]]

    def place(a, src, s, n):
        return out_refs[a].at[r, src, pl.ds(s, n)]

    def right(k, i, src, from_x=False):
        a, s, n = items[i]
        return pltpu.make_async_remote_copy(
            src_ref=x_refs[a].at[pl.ds(s, n)] if from_x else place(a, src, s, n),
            dst_ref=place(a, src, s, n),
            send_sem=send_r.at[k, i],
            recv_sem=recv_r.at[k, i],
            device_id={"exp": z + 1},
            device_id_type=MESH,
        )

    def left(k, i, src, from_x=False):
        a, s, n = items[i]
        return pltpu.make_async_remote_copy(
            src_ref=x_refs[a].at[pl.ds(s, n)] if from_x else place(a, src, s, n),
            dst_ref=place(a, src, s, n),
            send_sem=send_l.at[k, i],
            recv_sem=recv_l.at[k, i],
            device_id={"exp": z - 1},
            device_id_type=MESH,
        )

    def cross(k, i, src, from_x=False):
        a, s, n = items[i]
        return pltpu.make_async_remote_copy(
            src_ref=x_refs[a].at[pl.ds(s, n)] if from_x else place(a, src, s, n),
            dst_ref=place(a, src, s, n),
            send_sem=send_c.at[k, i],
            recv_sem=recv_c.at[k, i],
            device_id={"row": 1 - r},
            device_id_type=MESH,
        )

    def landed(k, i, src):
        a, s, n = items[i]
        return pltpu.make_async_remote_copy(
            src_ref=out_refs[a].at[1 - r, src, pl.ds(s, n)],
            dst_ref=out_refs[a].at[1 - r, src, pl.ds(s, n)],
            send_sem=send_c.at[k, i],
            recv_sem=recv_c.at[k, i],
            device_id={"row": 1 - r},
            device_id_type=MESH,
        )

    total = len(items)
    for i in range(total):

        @pl.when(has_r)
        def _():
            right(0, i, z, True).start()

        @pl.when(has_l)
        def _():
            left(0, i, z, True).start()

    for i in range(total):
        cross(0, i, z, True).start()
    own = [
        pltpu.make_async_copy(x_refs[a], out_refs[a].at[r, z], own_sem.at[a]) for a in range(count)
    ]
    for copy in own:
        copy.start()
    for k in range(nz - 1):
        for i in range(total):

            @pl.when(z - 1 - k >= 0)
            def _():
                right(k, i, z - 1 - k).wait_recv()

                @pl.when(has_r)
                def _():
                    right(k + 1, i, z - 1 - k).start()

                cross(1 + k, i, z - 1 - k).start()

            @pl.when(z + 1 + k < nz)
            def _():
                left(k, i, z + 1 + k).wait_recv()

                @pl.when(has_l)
                def _():
                    left(k + 1, i, z + 1 + k).start()

                cross(nz + k, i, z + 1 + k).start()

    for i in range(total):

        @pl.when(has_r)
        def _():
            right(0, i, z, True).wait_send()

        @pl.when(has_l)
        def _():
            left(0, i, z, True).wait_send()

        cross(0, i, z, True).wait_send()
        landed(0, i, z).wait_recv()
        for k in range(nz - 1):

            @pl.when(z - 1 - k >= 0)
            def _():
                @pl.when(has_r)
                def _():
                    right(k + 1, i, z - 1 - k).wait_send()

                cross(1 + k, i, z - 1 - k).wait_send()
                landed(1 + k, i, z - 1 - k).wait_recv()

            @pl.when(z + 1 + k < nz)
            def _():
                @pl.when(has_l)
                def _():
                    left(k + 1, i, z + 1 + k).wait_send()

                cross(nz + k, i, z + 1 + k).wait_send()
                landed(nz + k, i, z + 1 + k).wait_recv()

    for copy in own:
        copy.wait()


def line_gather(nz, arrays, counts, cid):
    pieces = [cuts(a.shape[0], n) for a, n in zip(arrays, counts)]
    total = sum(len(p) for p in pieces)
    count = len(arrays)
    sems = pltpu.SemaphoreType.DMA
    return pl.pallas_call(
        functools.partial(gather_kernel, nz, pieces, count),
        out_shape=[jax.ShapeDtypeStruct((2, nz) + a.shape, a.dtype) for a in arrays],
        in_specs=[ANY] * count,
        out_specs=[ANY] * count,
        scratch_shapes=[
            sems((nz, total)),
            sems((nz, total)),
            sems((nz, total)),
            sems((nz, total)),
            sems((2 * nz, total)),
            sems((2 * nz, total)),
            sems((count,)),
        ],
        compiler_params=params(collective_id=cid, has_side_effects=True),
        name=f"line_gather_{cid}",
    )(*arrays)


def scatter_kernel(nz, pieces, extra, *refs):
    if extra:
        part_ref, small_ref, out_ref, small_out = refs[:4]
        rest = refs[4:]
    else:
        part_ref, out_ref = refs[:2]
        rest = refs[2:]
    sib, rbuf, lbuf, sc_s, sc_r, sr_s, sr_r, sl_s, sl_r = rest[:9]
    r, z = lax.axis_index("row"), lax.axis_index("exp")
    has_l, has_r = z > 0, z < nz - 1
    barrier = pltpu.get_barrier_semaphore()
    if extra:
        sd_s, sd_r, own_sem = rest[9:]
        peers = [(a, s) for a in range(2) for s in range(nz) if (a, s) != (0, 0)]

        def peer(a, s):
            return {"row": lax.rem(r + a, 2), "exp": lax.rem(z + s, nz)}

        for a, s in peers:
            pl.semaphore_signal(barrier, inc=1, device_id=peer(a, s), device_id_type=MESH)
        pl.semaphore_wait(barrier, len(peers))
    else:

        @pl.when(has_l)
        def _():
            pl.semaphore_signal(barrier, inc=1, device_id={"exp": z - 1}, device_id_type=MESH)

        @pl.when(has_r)
        def _():
            pl.semaphore_signal(barrier, inc=1, device_id={"exp": z + 1}, device_id_type=MESH)

        pl.semaphore_signal(barrier, inc=1, device_id={"row": 1 - r}, device_id_type=MESH)
        pl.semaphore_wait(barrier, 1 + has_l.astype(jnp.int32) + has_r.astype(jnp.int32))

    def cross(d, i):
        s, n = pieces[i]
        return pltpu.make_async_remote_copy(
            src_ref=part_ref.at[1 - r, d, pl.ds(s, n)],
            dst_ref=sib.at[d, pl.ds(s, n)],
            send_sem=sc_s.at[d, i],
            recv_sem=sc_r.at[d, i],
            device_id={"row": 1 - r},
            device_id_type=MESH,
        )

    def right(d, i):
        s, n = pieces[i]
        return pltpu.make_async_remote_copy(
            src_ref=sib.at[d, pl.ds(s, n)],
            dst_ref=rbuf.at[d, pl.ds(s, n)],
            send_sem=sr_s.at[d, i],
            recv_sem=sr_r.at[d, i],
            device_id={"exp": z + 1},
            device_id_type=MESH,
        )

    def left(d, i):
        s, n = pieces[i]
        return pltpu.make_async_remote_copy(
            src_ref=sib.at[d, pl.ds(s, n)],
            dst_ref=lbuf.at[d, pl.ds(s, n)],
            send_sem=sl_s.at[d, i],
            recv_sem=sl_r.at[d, i],
            device_id={"exp": z - 1},
            device_id_type=MESH,
        )

    for k in range(nz - 1):
        for i in range(len(pieces)):

            @pl.when(nz - 1 - k > z)
            def _():
                cross(nz - 1 - k, i).start()

            @pl.when(k < z)
            def _():
                cross(k, i).start()

    for i in range(len(pieces)):
        cross(z, i).start()
    if extra:

        def tiny(a, s):
            to = peer(a, s)
            return pltpu.make_async_remote_copy(
                src_ref=small_ref.at[to["row"], to["exp"]],
                dst_ref=small_out.at[r, z],
                send_sem=sd_s.at[a, s],
                recv_sem=sd_r.at[a, s],
                device_id=to,
                device_id_type=MESH,
            )

        for a, s in peers:
            tiny(a, s).start()
        keep = pltpu.make_async_copy(small_ref.at[r, z], small_out.at[r, z], own_sem)
        keep.start()

    for k in range(nz - 1):
        for i, (s, n) in enumerate(pieces):
            rows = pl.ds(s, n)
            d = nz - 1 - k

            @pl.when(d > z)
            def _():
                cross(d, i).wait_recv()
                value = part_ref[r, d, rows].astype(F32) + sib[d, rows].astype(F32)

                @pl.when(has_l)
                def _():
                    right(d, i).wait_recv()
                    sib[d, rows] = (value + rbuf[d, rows].astype(F32)).astype(sib.dtype)

                @pl.when(jnp.logical_not(has_l))
                def _():
                    sib[d, rows] = value.astype(sib.dtype)

                right(d, i).start()

            @pl.when(k < z)
            def _():
                cross(k, i).wait_recv()
                value = part_ref[r, k, rows].astype(F32) + sib[k, rows].astype(F32)

                @pl.when(has_r)
                def _():
                    left(k, i).wait_recv()
                    sib[k, rows] = (value + lbuf[k, rows].astype(F32)).astype(sib.dtype)

                @pl.when(jnp.logical_not(has_r))
                def _():
                    sib[k, rows] = value.astype(sib.dtype)

                left(k, i).start()

    for i, (s, n) in enumerate(pieces):
        rows = pl.ds(s, n)
        cross(z, i).wait_recv()
        out_ref[rows] = part_ref[r, z, rows].astype(F32) + sib[z, rows].astype(F32)

        @pl.when(has_l)
        def _():
            right(z, i).wait_recv()
            out_ref[rows] = out_ref[rows] + rbuf[z, rows].astype(F32)

        @pl.when(has_r)
        def _():
            left(z, i).wait_recv()
            out_ref[rows] = out_ref[rows] + lbuf[z, rows].astype(F32)

    for i in range(len(pieces)):
        cross(z, i).wait_send()
        for k in range(nz - 1):

            @pl.when(nz - 1 - k > z)
            def _():
                cross(nz - 1 - k, i).wait_send()
                right(nz - 1 - k, i).wait_send()

            @pl.when(k < z)
            def _():
                cross(k, i).wait_send()
                left(k, i).wait_send()

    if extra:
        for a, s in peers:
            tiny(a, s).wait_send()
            came = {"row": lax.rem(r + a, 2), "exp": lax.rem(z + nz - s, nz)}
            pltpu.make_async_remote_copy(
                src_ref=small_ref.at[0, 0],
                dst_ref=small_out.at[came["row"], came["exp"]],
                send_sem=sd_s.at[a, s],
                recv_sem=sd_r.at[a, s],
                device_id=came,
                device_id_type=MESH,
            ).wait_recv()
        keep.wait()


def line_scatter(nz, part, chunks, cid, small=None):
    rows, width = part.shape[2:]
    pieces = cuts(rows, chunks)
    n = len(pieces)
    sems = pltpu.SemaphoreType.DMA
    extra = small is not None
    out_shape = [jax.ShapeDtypeStruct((rows, width), F32)]
    scratch = [pltpu.VMEM((nz, rows, width), BF16)] * 3 + [sems((nz, n))] * 6
    if extra:
        out_shape.append(jax.ShapeDtypeStruct(small.shape, F32))
        scratch += [sems((2, nz)), sems((2, nz)), sems]
    out = pl.pallas_call(
        functools.partial(scatter_kernel, nz, pieces, extra),
        out_shape=out_shape,
        in_specs=[VM] * (1 + extra),
        out_specs=[VM] * (1 + extra),
        scratch_shapes=scratch,
        compiler_params=params(collective_id=cid, has_side_effects=True),
        name=f"line_scatter_{cid}",
    )(*((part, small) if extra else (part,)))
    return out if extra else out[0]


def swap_halves(v):
    lane = lax.broadcasted_iota(jnp.int32, v.shape, 1)
    width = v.shape[1]
    ahead = pltpu.roll(v, width - HEAD // 2, 1)
    behind = pltpu.roll(v, HEAD // 2, 1)
    return jnp.where(lane % HEAD < HEAD // 2, ahead, behind)


def rotate(v, cos, sin):
    return v * cos + swap_halves(v) * sin


def project_kernel(x0, x1, x2, x3, gain, wq, wk, wv, cos_ref, sin_ref, n_ref, q_ref, k_ref, v_ref):
    c = lax.axis_index("col")
    rows_n = x0.shape[0]
    for j, x_ref in enumerate((x0, x1, x2, x3)):
        rows = pl.ds(pl.multiple_of(mate(c, j) * rows_n, rows_n), rows_n)
        x = x_ref[...].astype(F32)
        inv = lax.rsqrt(jnp.mean(x * x, axis=1, keepdims=True) + EPS)
        n = (x * inv * gain[...]).astype(BF16)
        n_ref[rows] = n
        cos, sin = cos_ref[rows], sin_ref[rows]
        q = dot(n, wq[...], 1, 0)
        for h in range(q.shape[1] // 128):
            rot = (rotate(q[:, h * 128 : h * 128 + 128], cos, sin) * HEAD**-0.5).astype(BF16)
            q_ref[2 * h, rows] = rot[:, :HEAD]
            q_ref[2 * h + 1, rows] = rot[:, HEAD:]
        k = dot(n, wk[...], 1, 0)
        v = dot(n, wv[...], 1, 0).astype(BF16)
        for h in range(k.shape[1] // 128):
            rot = rotate(k[:, h * 128 : h * 128 + 128], cos, sin).astype(BF16)
            k_ref[2 * h, rows] = rot[:, :HEAD]
            k_ref[2 * h + 1, rows] = rot[:, HEAD:]
            v_ref[2 * h, rows] = v[:, h * 128 : h * 128 + HEAD]
            v_ref[2 * h + 1, rows] = v[:, h * 128 + HEAD : h * 128 + 128]


def attention_scope(j, sc, st_ref, group_rows, bq, ratio):
    start = lax.axis_index("row") * group_rows
    st = jnp.concatenate([st_ref[0:1, :]] * ratio, axis=1)
    blk = sc[j, 0]
    at = start + blk * bq + lax.broadcasted_iota(jnp.int32, (1, bq), 1)
    at = jnp.concatenate([at] * ratio, axis=1)
    return start, st, at, blk


def attend_kernel(
    j, sc, q_ref, st_ref, ko, vo, kp, vp, wo, branch_ref, att_ref, o_ref, lse_ref
):
    heads, bq, _ = q_ref.shape
    groups, group_rows, _ = ko.shape
    ratio = heads // groups
    wide = ratio * bq
    start, st, at, blk = attention_scope(j, sc, st_ref, group_rows, bq, ratio)
    qs = [
        jnp.concatenate([q_ref[g * ratio + i] for i in range(ratio)], axis=0)
        for g in range(groups)
    ]
    place = lax.broadcasted_iota(jnp.int32, (BK, wide), 0)

    def step(k_in, v_in, block, base, carry, last):
        rows = pl.ds(pl.multiple_of(block * BK, BK), BK)
        key = place + (base + block * BK)
        ok = key >= st
        if last:
            ok = ok & (key <= at)
        out = []
        for g in range(groups):
            m, l, acc = carry[g]
            s = jnp.where(ok, dot(k_in[g, rows], qs[g], 1, 1), NEG)
            m_new = jnp.maximum(m, jnp.max(s, axis=0, keepdims=True))
            scale = jnp.exp(m - m_new)
            p = jnp.exp(s - m_new)
            l = l * scale + jnp.sum(p, axis=0, keepdims=True)
            acc = acc * scale + dot(v_in[g, rows], p.astype(BF16), 0, 0)
            out.append((m_new, l, acc))
        return tuple(out)

    carry = tuple(
        (
            jnp.full((1, wide), NEG, F32),
            jnp.zeros((1, wide), F32),
            jnp.zeros((HEAD, wide), F32),
        )
        for _ in range(groups)
    )
    carry = step(ko, vo, blk, start, carry, True)
    carry = lax.fori_loop(
        sc[j, 3], blk, lambda b, cr: step(ko, vo, b, start, cr, False), carry
    )
    carry = lax.fori_loop(
        sc[j, 1], sc[j, 2], lambda b, cr: step(kp, vp, b, 0, cr, False), carry
    )
    for g in range(groups):
        m, l, acc = carry[g]
        o = acc / l
        lse = m + jnp.log(l)
        for i in range(ratio):
            h = g * ratio + i
            o_ref[:, h * HEAD : (h + 1) * HEAD] = o[:, i * bq : (i + 1) * bq].T
            lse_ref[h : h + 1, :] = lse[:, i * bq : (i + 1) * bq]
    att = o_ref[...].astype(BF16)
    att_ref[...] = att
    branch_ref[...] = dot(att, wo[...], 1, 0).astype(BF16)


def attend_back_kernel(j, first, *refs):
    sc, q_ref, st_ref, ko, vo, kp, vp, wo, db_ref, att_ref, o_ref, lse_ref, cos_ref, sin_ref = refs[
        :14
    ]
    if first:
        dq_ref, dko, dkp, dwo = refs[14:]
    else:
        dko_in, dkp_in, dwo_in, dq_ref, dko, dkp, dwo = refs[14:]
    heads, bq, _ = q_ref.shape
    groups, group_rows, _ = ko.shape
    ratio = heads // groups
    wide = ratio * bq
    start, st, at, blk = attention_scope(j, sc, st_ref, group_rows, bq, ratio)
    db = db_ref[...]
    do = dot(db, wo[...], 1, 1).astype(BF16)
    dw = dot(att_ref[...], db, 0, 0)
    if first:
        dko[...] = jnp.zeros_like(dko)
        dkp[...] = jnp.zeros_like(dkp)
        dwo[...] = dw
    else:
        dko[...] = dko_in[...]
        dkp[...] = dkp_in[...]
        dwo[...] = dwo_in[...] + dw
    prod = (do.astype(F32) * o_ref[...]).T
    qs, dos, lses, deltas = [], [], [], []
    for g in range(groups):
        hs = range(g * ratio, (g + 1) * ratio)
        qs.append(jnp.concatenate([q_ref[h] for h in hs], axis=0))
        dos.append(jnp.concatenate([do[:, h * HEAD : (h + 1) * HEAD] for h in hs], axis=0))
        lses.append(jnp.concatenate([lse_ref[h : h + 1, :] for h in hs], axis=1))
        deltas.append(
            jnp.concatenate(
                [jnp.sum(prod[h * HEAD : (h + 1) * HEAD], axis=0, keepdims=True) for h in hs],
                axis=1,
            )
        )
    place = lax.broadcasted_iota(jnp.int32, (BK, wide), 0)

    def step(k_in, v_in, acc_ref, block, base, carry, last):
        rows = pl.ds(pl.multiple_of(block * BK, BK), BK)
        key = place + (base + block * BK)
        ok = key >= st
        if last:
            ok = ok & (key <= at)
        out, dks, dvs = [], [], []
        for g in range(groups):
            k, v = k_in[g, rows], v_in[g, rows]
            s = dot(k, qs[g], 1, 1)
            p = jnp.exp(jnp.where(ok, s - lses[g], NEG))
            dp = dot(v, dos[g], 1, 1)
            ds = (p * (dp - deltas[g])).astype(BF16)
            dks.append(dot(ds, qs[g], 1, 0))
            dvs.append(dot(p.astype(BF16), dos[g], 1, 0))
            out.append(carry[g] + dot(k, ds, 0, 0))
        acc_ref[rows] = acc_ref[rows] + jnp.concatenate(dks + dvs, axis=1)
        return tuple(out)

    carry = tuple(jnp.zeros((HEAD, wide), F32) for _ in range(groups))
    carry = step(ko, vo, dko, blk, start, carry, True)
    carry = lax.fori_loop(
        sc[j, 3], blk, lambda b, cr: step(ko, vo, dko, b, start, cr, False), carry
    )
    carry = lax.fori_loop(
        sc[j, 1], sc[j, 2], lambda b, cr: step(kp, vp, dkp, b, 0, cr, False), carry
    )
    rows = pl.ds(pl.multiple_of(blk * bq, bq), bq)
    cos, sin = cos_ref[rows], sin_ref[rows]
    for h in range(0, heads, 2):
        pair = jnp.concatenate(
            [
                carry[i // ratio][:, (i % ratio) * bq : (i % ratio + 1) * bq].T
                for i in (h, h + 1)
            ],
            axis=1,
        )
        pair = pair * HEAD**-0.5
        dq_ref[:, h * HEAD : (h + 2) * HEAD] = rotate(pair, cos, -sin).astype(BF16)


def finish_kernel(
    x0, x1, x2, x3, q0, q1, q2, q3, dkv, came, cos_ref, sin_ref, wq, wk, wv,
    n0, n1, n2, n3, dqkv_ref, gain_ref,
):
    c = lax.axis_index("col")
    rows_n, model = x0.shape
    width_q, width_k = wq.shape[1], wk.shape[1]
    total = jnp.zeros((1, model), F32)
    for j, (x_ref, q_ref, n_ref) in enumerate(
        zip((x0, x1, x2, x3), (q0, q1, q2, q3), (n0, n1, n2, n3))
    ):
        rows = pl.ds(pl.multiple_of(mate(c, j) * rows_n, rows_n), rows_n)
        both = dkv[rows] + came[rows].astype(F32)
        dk = rotate(both[:, :width_k], cos_ref[rows], -sin_ref[rows]).astype(BF16)
        dv = both[:, width_k:].astype(BF16)
        dq = q_ref[...]
        dqkv_ref[rows, :width_q] = dq
        dqkv_ref[rows, width_q : width_q + width_k] = dk
        dqkv_ref[rows, width_q + width_k :] = dv
        dn = dot(dq, wq[...], 1, 1) + dot(dk, wk[...], 1, 1) + dot(dv, wv[...], 1, 1)
        n_ref[...] = dn.astype(BF16)
        x = x_ref[...].astype(F32)
        inv = lax.rsqrt(jnp.mean(x * x, axis=1, keepdims=True) + EPS)
        total = total + jnp.sum(dn * (x * inv), axis=0, keepdims=True)
    gain_ref[...] = total


def expert_kernel(
    cap, n_row, sc, n_ref, do_ref, rank_ref, wr_ref, wg, wu, wd,
    y_ref, dn_ref, dg_ref, gate_ref, keep_a, send_a, keep_b, send_b,
    x32, d32, slot_gate, xb, act_s, dgu_s, dy_s, gu32, dw32,
):
    e = pl.program_id(0)
    blocks, rows_n, model = n_ref.shape
    hidden = wg.shape[2]
    slots = blocks * cap
    ge = sc[0] + e
    c = sc[2]

    @pl.when(e == 0)
    def _():
        for s in range(blocks):
            logits = dot(wr_ref[...], n_ref[s], 1, 1)
            named = rank_ref[s] >= 0.0
            logits = jnp.where(named, logits, NEG)
            top = jnp.max(logits, axis=0, keepdims=True)
            raised = jnp.where(named, jnp.exp(logits - top), 0.0)
            gate_ref[s] = raised / jnp.sum(raised, axis=0, keepdims=True)

    slot = lax.broadcasted_iota(jnp.int32, (cap, rows_n), 0).astype(F32)
    for s in range(blocks):
        pick = slot == rank_ref[s, pl.ds(ge, 1), :]
        one = jnp.where(pick, 1.0, 0.0).astype(BF16)
        rows = slice(s * cap, (s + 1) * cap)
        x32[rows] = dot(one, n_ref[s], 1, 0)
        d32[rows] = dot(one, do_ref[s], 1, 0)
        slot_gate[rows] = jnp.sum(
            jnp.where(pick, gate_ref[s, pl.ds(ge, 1), :], 0.0), axis=1, keepdims=True
        )

    tile = slots // 2
    for t in range(2):
        rows = slice(t * tile, (t + 1) * tile)
        x = x32[rows].astype(BF16)
        xb[rows] = x
        gate = dot(x, wg[0], 1, 0)
        up = dot(x, wu[0], 1, 0)
        sig = 1.0 / (1.0 + jnp.exp(-gate))
        silu = gate * sig
        act = (silu * up).astype(BF16)
        act_s[rows] = act
        y = dot(act, wd[0], 1, 0).astype(BF16)
        y_ref[0, rows] = y
        d = d32[rows]
        slot_gate_t = slot_gate[rows]
        dy = (d * slot_gate_t).astype(BF16)
        dy_s[rows] = dy
        slot_gate[rows] = jnp.sum(d * y.astype(F32), axis=1, keepdims=True)
        dact = dot(dy, wd[0], 1, 1)
        dgate = (dact * up * sig * (1.0 + gate * (1.0 - sig))).astype(BF16)
        dup = (dact * silu).astype(BF16)
        dgu_s[rows, :hidden] = dgate
        dgu_s[rows, hidden:] = dup
        dn_ref[0, rows] = (dot(dgate, wg[0], 1, 1) + dot(dup, wu[0], 1, 1)).astype(BF16)

    for s in range(blocks):
        pick = slot == rank_ref[s, pl.ds(ge, 1), :]
        back = slot_gate[s * cap : (s + 1) * cap]
        dg_ref[s, pl.ds(e, 1), :] = jnp.sum(jnp.where(pick, back, 0.0), axis=0, keepdims=True)

    gu32[...] = dot(xb[...], dgu_s[...], 0, 0)
    dw32[...] = dot(act_s[...], dy_s[...], 0, 0)
    half = dw32.shape[1] // 2
    chunk = model // (n_row * 4)
    part = hidden // (n_row * 4)

    def store(keep, send, order):
        for slot_at, j in enumerate(order):
            to, at = (keep, slot_at) if slot_at < 2 else (send, slot_at - 2)
            for row in range(n_row):
                who = row * 4 + mate(c, j)
                first = pl.ds(pl.multiple_of(who * chunk, chunk), chunk)
                to[0, at, row] = gu32[first, :hidden].astype(BF16)
                to[1, at, row] = gu32[first, hidden:].astype(BF16)
                second = pl.ds(pl.multiple_of(who * part, part), part)
                to[2, at, row, :part] = dw32[second, :half].astype(BF16)
                to[2, at, row, part:] = dw32[second, half:].astype(BF16)

    @pl.when(e == 0)
    def _():
        store(keep_a, send_a, (0, 2, 1, 3))

    @pl.when(e == 1)
    def _():
        store(keep_b, send_b, (0, 1, 2, 3))


def experts(cap, n_row, scalars, tokens, grads, ranks, router_t, w_gate, w_up, w_down):
    blocks, rows_n, model = tokens.shape
    total = ranks.shape[1]
    hidden = w_gate.shape[2]
    slots = blocks * cap
    chunk = model // (n_row * 4)
    once = pl.Buffered(1)

    def fixed(shape):
        return pl.BlockSpec(shape, lambda e, sc: (0,) * len(shape), pipeline_mode=once)

    def weight(a, b):
        return pl.BlockSpec((1, a, b), lambda e, sc: (sc[1] + e, 0, 0))

    grad_shape = (3, 2, n_row, chunk, hidden)
    grad = jax.ShapeDtypeStruct(grad_shape, BF16)
    flops = 2 * slots * model * hidden * 9 + 4 * slots * rows_n * model
    return pl.pallas_call(
        functools.partial(expert_kernel, cap, n_row),
        grid_spec=pltpu.PrefetchScalarGridSpec(
            num_scalar_prefetch=1,
            grid=(2,),
            in_specs=[
                fixed(tokens.shape),
                fixed(grads.shape),
                fixed(ranks.shape),
                fixed(router_t.shape),
                weight(model, hidden),
                weight(model, hidden),
                weight(hidden, model),
            ],
            out_specs=[
                pl.BlockSpec((1, slots, model), lambda e, sc: (e, 0, 0)),
                pl.BlockSpec((1, slots, model), lambda e, sc: (e, 0, 0)),
                fixed((blocks, 2, rows_n)),
                fixed((blocks, total, rows_n)),
                fixed(grad_shape),
                fixed(grad_shape),
                fixed(grad_shape),
                fixed(grad_shape),
            ],
            scratch_shapes=[
                pltpu.VMEM((slots, model), F32),
                pltpu.VMEM((slots, model), F32),
                pltpu.VMEM((slots, 1), F32),
                pltpu.VMEM((slots, model), BF16),
                pltpu.VMEM((slots, hidden), BF16),
                pltpu.VMEM((slots, 2 * hidden), BF16),
                pltpu.VMEM((slots, model), BF16),
                pltpu.VMEM((model, 2 * hidden), F32),
                pltpu.VMEM((hidden, model), F32),
            ],
        ),
        out_shape=[
            jax.ShapeDtypeStruct((2, slots, model), BF16),
            jax.ShapeDtypeStruct((2, slots, model), BF16),
            jax.ShapeDtypeStruct((blocks, 2, rows_n), F32),
            jax.ShapeDtypeStruct((blocks, total, rows_n), F32),
            grad,
            grad,
            grad,
            grad,
        ],
        compiler_params=params(dimension_semantics=("arbitrary",)),
        cost_estimate=cost(2 * flops, 6 * model * hidden * 4 + 16 * slots * model, slots * hidden),
        name="experts",
    )(scalars, tokens, grads, ranks, router_t, w_gate, w_up, w_down)


def combine_kernel(cap, count, weighted, sc, rank_ref, gate_ref, *refs):
    s_refs, out_ref = refs[:-1], refs[-1]
    rows_n = rank_ref.shape[2]
    slot = lax.broadcasted_iota(jnp.int32, (cap, rows_n), 0).astype(F32)
    for b in range(2):
        picks, values = [], []
        for e in range(count):
            ge = pl.ds(sc[0] + e, 1)
            pick = slot == rank_ref[b, ge, :]
            picks.append(jnp.where(pick, gate_ref[b, ge, :] if weighted else 1.0, 0.0))
            src = s_refs[e // 2][e % 2].astype(F32)
            values.append(src[b * cap : (b + 1) * cap])
        out_ref[b] = dot(
            jnp.concatenate(picks, axis=0).astype(BF16),
            jnp.concatenate(values, axis=0).astype(BF16),
            0,
            0,
        ).astype(BF16)


def combine(cap, scalars, ranks, gates, slot_values, weighted):
    blocks, total, rows_n = ranks.shape
    model = slot_values[0].shape[2]
    count = 2 * len(slot_values)
    return pl.pallas_call(
        functools.partial(combine_kernel, cap, count, weighted),
        grid_spec=pltpu.PrefetchScalarGridSpec(
            num_scalar_prefetch=1,
            grid=(blocks // 2,),
            in_specs=[pl.BlockSpec((2, total, rows_n), lambda b, sc: (b, 0, 0))] * 2
            + [pl.BlockSpec((2, 2 * cap, model), lambda b, sc: (0, b, 0))] * len(slot_values),
            out_specs=pl.BlockSpec((2, rows_n, model), lambda b, sc: (b, 0, 0)),
        ),
        out_shape=jax.ShapeDtypeStruct((blocks, rows_n, model), BF16),
        compiler_params=params(dimension_semantics=("arbitrary",)),
        cost_estimate=cost(
            2 * blocks * rows_n * count * cap * model, 4 * blocks * count * cap * model
        ),
        name="combine",
    )(scalars, ranks, gates, *slot_values)


def angle_tables(offset, rows):
    places = (offset + jnp.arange(rows, dtype=jnp.int32)).astype(F32)
    frequency = THETA ** (-(jnp.arange(HEAD // 2).astype(F32) * 2.0 / HEAD))
    angles = places[:, None] * frequency[None, :]
    cos, sin = jnp.cos(angles), jnp.sin(angles)
    return (
        jnp.concatenate([cos, cos, cos, cos], axis=1),
        jnp.concatenate([-sin, sin, -sin, sin], axis=1),
    )


def norm_back(grad, xhat, inv, gain):
    scaled = grad * gain
    return inv * (scaled - xhat * jnp.mean(scaled * xhat, axis=-1, keepdims=True))


def whole_call(kernel, out_shape, args, name, specs=None, flops=0, **kw):
    nbytes = sum(a.size * a.dtype.itemsize for a in args)
    return pl.pallas_call(
        kernel,
        out_shape=out_shape,
        in_specs=specs or [VM] * len(args),
        out_specs=[VM] * len(out_shape),
        compiler_params=params(),
        cost_estimate=cost(flops, nbytes),
        name=name,
        **kw,
    )(*args)


def local(
    tokens, seg_ids, routes, priority, cotangent, norm1_gain, w_query, key_projection,
    value_projection, w_out, norm2_gain, w_router, w_gate, w_up, w_down,
):
    sds = jax.ShapeDtypeStruct
    n_row, n_col, nz = (lax.axis_size(a) for a in ("row", "col", "exp"))
    assert n_col == 4
    paired = n_row == 2
    r, c, z = (lax.axis_index(a) for a in ("row", "col", "exp"))
    own, model = tokens.shape[1:]
    group = own * n_col
    length = seg_ids.shape[1]
    total = w_router.shape[1]
    plane = w_gate.shape[0]
    hidden = w_gate.shape[2]
    top = routes.shape[2]
    cap = 9 * own * top // (8 * total)
    share = 2 if paired else 1
    mine = plane // share
    heads, kv_heads = w_query.shape[1] // HEAD, key_projection.shape[1] // HEAD
    width_k = kv_heads * HEAD
    gain1 = norm1_gain.astype(F32)[None]
    gain2 = norm2_gain.astype(F32)[None]

    x_own = tokens[0]
    xs = [x_own] + [col_swap(x_own, j) for j in (1, 2, 3)]

    route = routes[0]
    named = (route[None, :, :] == jnp.arange(total, dtype=jnp.int32)[:, None, None]).any(-1)
    prio = priority[0]
    earlier = (prio[:, None] < prio[None, :]).astype(BF16)
    before = jnp.dot(named.astype(BF16), earlier, preferred_element_type=F32)
    rank_own = jnp.where(named, before, -1.0)
    cot = cotangent[0]
    if paired:
        grads, ranks = line_gather(nz, [cot, rank_own], [4, 1], 1)
        grads, ranks = grads.reshape(2 * nz, own, model), ranks.reshape(2 * nz, total, own)
    else:
        grads = lax.all_gather(cot, "exp")
        ranks = lax.all_gather(rank_own, "exp")

    cos, sin = angle_tables(r * group, group)
    segment = seg_ids[0]
    own_seg = lax.dynamic_slice_in_dim(segment, r * group, group, 0)
    starts = jnp.sum((segment[None, :] < own_seg[:, None]).astype(jnp.int32), axis=1)
    blks = jnp.stack([mate(c, j) for j in range(4)])
    first = starts[blks * own] // BK
    base = r * (group // BK)
    table = jnp.stack(
        [
            blks,
            jnp.minimum(first, base),
            jnp.full((4,), base, jnp.int32),
            jnp.maximum(first - base, 0),
        ],
        axis=1,
    ).astype(jnp.int32)
    starts = starts.astype(jnp.int32)[None]
    normed1, q4, k2, v2 = whole_call(
        project_kernel,
        [
            sds((group, model), BF16),
            sds((heads, group, HEAD), BF16),
            sds((kv_heads, group, HEAD), BF16),
            sds((kv_heads, group, HEAD), BF16),
        ],
        (*xs, gain1, w_query, key_projection, value_projection, cos, sin),
        "project",
        flops=2 * group * model * (heads + 2 * kv_heads) * HEAD,
    )
    if paired:
        k_prev, v_prev = (lax.ppermute(t, "row", [(0, 1)]) for t in (k2, v2))
    else:
        k_prev, v_prev = (lax.all_gather(t, "row", axis=1, tiled=True) for t in (k2, v2))
    before_rows = k_prev.shape[1]

    def blocked(shape, at):
        def index(i, sc, j):
            return tuple(sc[j, 0] if a else 0 for a in at)

        return lambda j: pl.BlockSpec(shape, lambda i, sc: index(i, sc, j))

    def full(shape):
        return pl.BlockSpec(shape, lambda i, sc: (0,) * len(shape))

    q_spec = blocked((heads, own, HEAD), (0, 1, 0))
    st_spec = blocked((1, own), (0, 1))
    att_flops = 4 * heads * own * (group + 512) * HEAD
    branches, atts, os_, lses = [None] * 4, [None] * 4, [None] * 4, [None] * 4
    for j in (3, 1, 2, 0):
        branches[j], atts[j], os_[j], lses[j] = pl.pallas_call(
            functools.partial(attend_kernel, j),
            grid_spec=pltpu.PrefetchScalarGridSpec(
                num_scalar_prefetch=1,
                grid=(1,),
                in_specs=[q_spec(j), st_spec(j)]
                + [full(t.shape) for t in (k2, v2, k_prev, v_prev, w_out)],
                out_specs=[
                    full((own, model)),
                    full((own, heads * HEAD)),
                    full((own, heads * HEAD)),
                    full((8, own)),
                ],
            ),
            out_shape=[
                sds((own, model), BF16),
                sds((own, heads * HEAD), BF16),
                sds((own, heads * HEAD), F32),
                sds((8, own), F32),
            ],
            compiler_params=params(dimension_semantics=("arbitrary",)),
            cost_estimate=cost(att_flops + 2 * own * model * heads * HEAD, 4 << 20, heads * own * group),
            name="attend",
        )(table, q4, starts, k2, v2, k_prev, v_prev, w_out)
    branch = branches[0].astype(F32)
    for j in (3, 1, 2):
        branch = branch + col_swap(branches[j], j).astype(F32)
    x_f = x_own.astype(F32)
    hidden_state = x_f + branch
    inv2 = lax.rsqrt(jnp.mean(hidden_state * hidden_state, axis=-1, keepdims=True) + EPS)
    xhat2 = hidden_state * inv2
    normed2 = (xhat2 * gain2).astype(BF16)

    if paired:
        (arrived,) = line_gather(nz, [normed2], [4], 2)
        arrived = arrived.reshape(2 * nz, own, model)
    else:
        arrived = lax.all_gather(normed2, "exp")
    blocks = share * nz
    offset = r * mine if paired else 0
    router_t = w_router.T
    runs = []
    for first_e in range(0, mine, 2):
        scalars = jnp.stack(
            [z * plane + offset + first_e, jnp.asarray(offset + first_e), c]
        ).astype(jnp.int32)
        runs.append(
            experts(cap, n_row, scalars, arrived, grads, ranks, router_t, w_gate, w_up, w_down)
        )
    gates = runs[0][3]
    base_sc = jnp.stack([z * plane + offset]).astype(jnp.int32)
    back_part = combine(cap, base_sc, ranks, gates, [run[1] for run in runs], False)
    mix_part = combine(cap, base_sc, ranks, gates, [run[0] for run in runs], True)
    dgs = jnp.concatenate([run[2] for run in runs], axis=1)
    if paired:
        dgs = jnp.pad(dgs, ((0, 0), (0, 8 - mine), (0, 0))).reshape(2, nz, 8, own)
        dn2, dg_all = line_scatter(
            nz, back_part.reshape(2, nz, own, model), 4, 3, small=dgs
        )
        dgates = jnp.transpose(dg_all[:, :, :mine], (1, 0, 2, 3)).reshape(total, own)
        gate_own = lax.dynamic_slice(gates, (r * nz + z, 0, 0), (1, total, own))[0]
    else:
        dn2 = lax.psum_scatter(back_part, "exp", scatter_dimension=0).astype(F32)
        dgates = lax.all_to_all(dgs, "exp", 0, 0).reshape(total, own)
        gate_own = lax.dynamic_slice(gates, (z, 0, 0), (1, total, own))[0]

    finals = []
    for run in runs:
        keep_a, send_a, keep_b, send_b = run[4:]
        if paired:
            for keep, send, one, two in ((keep_a, send_a, 1, 2), (keep_b, send_b, 2, 1)):
                came = col_swap(send, one)
                on = (keep[:, 1].astype(F32) + came[:, 1].astype(F32)).astype(BF16)
                last = col_swap(on, two)
                finals.append((keep[:, 0], came[:, 0], last))
        else:
            for keep, send, order in ((keep_a, send_a, (0, 2, 1, 3)), (keep_b, send_b, (0, 1, 2, 3))):
                parts = [keep[:, 0], keep[:, 1], send[:, 0], send[:, 1]]
                parts = [parts[order.index(j)] for j in range(4)]
                stacked = jnp.stack(parts, axis=2)
                stacked = stacked[:, :, jnp.stack([mate(c, j) for j in range(4)])]
                flat = stacked.reshape(3, n_row * 4, stacked.shape[3], hidden)
                got = lax.psum_scatter(flat, ("row", "col"), scatter_dimension=1)
                finals.append(got.astype(F32))

    dout = cot.astype(F32)
    dlogits = gate_own * (dgates - jnp.sum(gate_own * dgates, axis=0, keepdims=True))
    router_back = lax.dot_general(
        dlogits, router_t.astype(F32), (((0,), (0,)), ((), ())), precision=HIGH
    )
    dnormed2 = dn2 + router_back
    dhidden = dout + norm_back(dnormed2, xhat2, inv2, gain2)
    dbranch = dhidden.astype(BF16)
    dbs = [dbranch] + [col_swap(dbranch, j) for j in (1, 2, 3)]
    router_grad = lax.dot_general(
        normed2.astype(F32), dlogits, (((0,), (1,)), ((), ())), precision=HIGH
    )
    gain2_part = jnp.sum(dnormed2 * xhat2, axis=0)

    dqs, state = [None] * 4, ()
    for j in range(4):
        args = (
            table, q4, starts, k2, v2, k_prev, v_prev, w_out, dbs[j], atts[j], os_[j], lses[j],
            cos, sin,
        )
        specs = [q_spec(j), st_spec(j)] + [full(t.shape) for t in args[3:] + tuple(state)]
        out_shape = [
            sds((own, heads * HEAD), BF16),
            sds((group, 2 * width_k), F32),
            sds((before_rows, 2 * width_k), F32),
            sds((heads * HEAD, model), F32),
        ]
        out = pl.pallas_call(
            functools.partial(attend_back_kernel, j, j == 0),
            grid_spec=pltpu.PrefetchScalarGridSpec(
                num_scalar_prefetch=1,
                grid=(1,),
                in_specs=specs,
                out_specs=[full(s.shape) for s in out_shape],
            ),
            out_shape=out_shape,
            input_output_aliases={} if j == 0 else {14: 1, 15: 2, 16: 3},
            compiler_params=params(dimension_semantics=("arbitrary",)),
            cost_estimate=cost(5 * att_flops // 2, 6 << 20, heads * own * group),
            name="attend_back",
        )(*args, *state)
        dqs[j], state = out[0], tuple(out[1:])
    dkv, dkv_prev, dw_out = state
    if paired:
        came = lax.ppermute(dkv_prev.astype(BF16), "row", [(1, 0)])
    else:
        spread = dkv_prev.at[:].get()
        at = r * group
        spread = lax.dynamic_update_slice_in_dim(
            spread, lax.dynamic_slice_in_dim(spread, at, group, 0) + dkv, at, 0
        )
        dkv = lax.psum_scatter(spread.astype(BF16), "row", scatter_dimension=0, tiled=True).astype(F32)
        came = jnp.zeros(dkv.shape, BF16)
    width = (heads + 2 * kv_heads) * HEAD
    *dns, dqkv, gain1_part = whole_call(
        finish_kernel,
        [sds((own, model), BF16)] * 4 + [sds((group, width), BF16), sds((1, model), F32)],
        (*xs, *dqs, dkv, came, cos, sin, w_query, key_projection, value_projection),
        "finish",
        flops=2 * group * model * width,
    )
    dn1 = dns[0].astype(F32)
    for j in (3, 1, 2):
        dn1 = dn1 + col_swap(dns[j], j).astype(F32)
    dw_qkv = lax.dot_general(
        normed1, dqkv, (((0,), (0,)), ((), ())), preferred_element_type=F32
    )

    cols = model // 4
    small = jnp.concatenate([router_grad.T, gain2_part[None], gain1_part], axis=0)

    def piece(j):
        return lax.dynamic_slice(small, (0, mate(c, j) * cols), (small.shape[0], cols))

    small_sum = piece(0)
    for j in (1, 2, 3):
        small_sum = small_sum + col_swap(piece(j), j)
    if paired:
        half = model // 2
        lines = -(-small_sum.size // half)
        flat = jnp.pad(small_sum.reshape(-1), (0, lines * half - small_sum.size))
        packed = jnp.concatenate(
            [
                dw_qkv.astype(BF16).reshape(-1, half),
                dw_out[:, :half].astype(BF16),
                dw_out[:, half:].astype(BF16),
                flat.astype(BF16).reshape(lines, half),
            ],
            axis=0,
        )
        unit = 2 * nz * 16
        rows = -(-packed.shape[0] // unit) * unit
        packed = jnp.pad(packed, ((0, rows - packed.shape[0]), (0, 0)))
        mine_sum = line_scatter(nz, packed.reshape(2, nz, rows // (2 * nz), half), 2, 4)
        (summed,) = line_gather(nz, [mine_sum.astype(BF16)], [2], 5)
        summed = summed.reshape(rows, half)
        n_qkv = model * width // half
        n_out = heads * HEAD
        s_qkv = summed[:n_qkv].reshape(model, width).astype(F32)
        s_out = jnp.concatenate(
            [summed[n_qkv : n_qkv + n_out], summed[n_qkv + n_out : n_qkv + 2 * n_out]], axis=1
        ).astype(F32)
        s_small = summed[n_qkv + 2 * n_out : n_qkv + 2 * n_out + lines].reshape(-1)
        s_small = s_small[: small_sum.size].reshape(small_sum.shape).astype(F32)
    else:
        s_qkv, s_out, s_small = lax.psum((dw_qkv, dw_out, small_sum), ("row", "exp"))
    width_q = heads * HEAD

    chunk = model // (n_row * 4)
    if paired:
        ours, theirs = [], []
        for keep, came_, last in finals:
            def pick(row):
                return sum(
                    lax.dynamic_index_in_dim(t, row, 1, keepdims=False).astype(F32)
                    for t in (keep, came_, last)
                )
            ours.append(pick(r))
            theirs.append(pick(1 - r).astype(BF16))
        ours, got = jnp.stack(ours, axis=1), row_swap(jnp.stack(theirs, axis=1)).astype(F32)
        grads_e = jnp.where(
            r == 0, jnp.concatenate([ours, got], axis=1), jnp.concatenate([got, ours], axis=1)
        )
    else:
        grads_e = jnp.stack(finals, axis=1)
    part = chunk // 2
    down = jnp.concatenate([grads_e[2][:, :part], grads_e[2][:, part:]], axis=2)

    mix = mix_part
    if paired:
        mix = mix.reshape(2, nz, own, model)
        here = lax.dynamic_index_in_dim(mix, r, 0, keepdims=False)
        away = lax.dynamic_index_in_dim(mix, 1 - r, 0, keepdims=False)
        pair = (here.astype(F32) + row_swap(away).astype(F32)).astype(BF16)
        mixture = lax.dynamic_index_in_dim(pair, z, 0, keepdims=False).astype(F32)
        for s in range(1, nz):
            to = lax.rem(z + s, nz)
            send = lax.dynamic_index_in_dim(pair, to, 0, keepdims=False)
            mixture = mixture + lax.ppermute(
                send, "exp", [(i, (i + s) % nz) for i in range(nz)]
            ).astype(F32)
    else:
        mixture = lax.psum_scatter(mix, "exp", scatter_dimension=0).astype(F32)
    output = (hidden_state + mixture).astype(BF16)
    inv1 = lax.rsqrt(jnp.mean(x_f * x_f, axis=-1, keepdims=True) + EPS)
    input_gradient = dhidden + norm_back(dn1, x_f * inv1, inv1, gain1)
    return (
        output[None],
        input_gradient[None],
        s_small[total + 1],
        s_qkv[:, :width_q],
        s_qkv[:, width_q : width_q + width_k],
        s_qkv[:, width_q + width_k :],
        s_out,
        s_small[total],
        s_small[:total].T,
        grads_e[0],
        grads_e[1],
        down,
    )


def solution(mesh):
    in_specs = (
        P("exp", ("row", "col"), None),
        P("exp", None),
        P("exp", ("row", "col"), None),
        P("exp", ("row", "col")),
        P("exp", ("row", "col"), None),
        P(),
        P(None, "col"),
        P(None, "col"),
        P(None, "col"),
        P("col", None),
        P(),
        P(),
        P("exp", None, None),
        P("exp", None, None),
        P("exp", None, None),
    )
    out_specs = (
        P("exp", ("row", "col"), None),
        P("exp", ("row", "col"), None),
        P("col"),
        P(None, "col"),
        P(None, "col"),
        P(None, "col"),
        P("col", None),
        P("col"),
        P("col", None),
        P("exp", ("row", "col"), None),
        P("exp", ("row", "col"), None),
        P("exp", ("row", "col"), None),
    )
    return jax.shard_map(local, mesh=mesh, in_specs=in_specs, out_specs=out_specs, check_vma=False)
```
